8 devices in a mesh: dp: 1 (over z), tp: 2 (over y), sp: 4 (over x, core).
Axes of the slice: x: 2, y: 2, z: 1, core: 2. Of those that a mesh axis runs over, the one named last changes fastest.
Arguments:
- tok_emb: bfloat16 [4, 32, 1536], P(None, 'dp')
- lengths: int32 [32], P('dp')
- key_cache: bfloat16 [2, 32, 4096, 2, 128], P(None, 'dp', 'sp', 'tp')
- val_cache: bfloat16 [2, 32, 4096, 2, 128], P(None, 'dp', 'sp', 'tp')
- gain_attn: bfloat16 [2, 1536], replicated
- gain_mlp: bfloat16 [2, 1536], replicated
- w_query: bfloat16 [2, 1536, 1536], P(None, None, 'tp')
- w_key: bfloat16 [2, 1536, 256], P(None, None, 'tp')
- w_value: bfloat16 [2, 1536, 256], P(None, None, 'tp')
- w_out: bfloat16 [2, 1536, 1536], P(None, 'tp')
- w_gate: bfloat16 [2, 1536, 8960], P(None, None, 'tp')
- w_up: bfloat16 [2, 1536, 8960], P(None, None, 'tp')
- w_down: bfloat16 [2, 8960, 1536], P(None, 'tp')
Outputs:
- output 1: bfloat16 [4, 32, 1536], P(None, 'dp')
- output 2: bfloat16 [2, 32, 4096, 2, 128], P(None, 'dp', 'sp', 'tp')
- output 3: bfloat16 [2, 32, 4096, 2, 128], P(None, 'dp', 'sp', 'tp')
All inputs are finite; a program needn't handle non-finite values.
Results may differ from the reference program's by a relative error of at most 0.0148625.
Values sent between devices are 32-bit elements.
A program may use at most 1 GiB of HBM per device.

```python
import math
import jax
import jax.numpy as jnp
from jax import lax

N_STEPS = 4
N_LAYERS = 2
SEQ_BATCH = 32
LOC_LEN = 1024
SP_SIZE = 4
D_MODEL = 1536
N_HEADS = 12
KV_HEADS = 2
HEAD_DIM = 128
FF_DIM = 8960
CACHE_LEN = LOC_LEN * SP_SIZE
GROUP_SIZE = N_HEADS // KV_HEADS
EPS = 1e-5
ROPE_BASE = 500000.0


def draw_lengths(len_key, perm_key):
    drawn_len = jax.random.randint(len_key, (SEQ_BATCH,), CACHE_LEN // 2, CACHE_LEN - N_STEPS + 1)
    perm_ids = jax.random.permutation(perm_key, SEQ_BATCH)
    lengths = jnp.where(perm_ids == 0, CACHE_LEN - N_STEPS, jnp.where(perm_ids == 1, CACHE_LEN // 2, drawn_len))
    return lengths.astype(jnp.int32)


def draw_scales():
    score_var = max(math.log(CACHE_LEN / 32.0), 1.0)
    plant_gain = (math.log(CACHE_LEN) + 0.5 * score_var) / math.sqrt(HEAD_DIM)
    key_scale = math.sqrt(score_var / (1.0 + plant_gain * plant_gain))
    return plant_gain, key_scale


def setup_inputs(seed: int = 0, part: int = 0) -> dict:
    plant_gain, key_scale = draw_scales()
    part_keys = jax.random.split(jax.random.fold_in(jax.random.key(seed), part), 6)
    weight_keys = jax.random.split(jax.random.key(seed + 1), 9)
    common = jax.random.normal(part_keys[0], (SEQ_BATCH, D_MODEL), jnp.float32)
    step_noise = jax.random.normal(part_keys[1], (N_STEPS, SEQ_BATCH, D_MODEL), jnp.float32)
    tok_emb = ((common[None] + 0.4 * step_noise) / math.sqrt(1.16)).astype(jnp.bfloat16)
    lengths = draw_lengths(part_keys[2], part_keys[3])
    cache_shape = (N_LAYERS, SEQ_BATCH, CACHE_LEN, KV_HEADS, HEAD_DIM)
    key_cache = (key_scale * jax.random.normal(part_keys[4], cache_shape, jnp.float32)).astype(jnp.bfloat16)
    val_cache = jax.random.normal(part_keys[5], cache_shape, jnp.float32).astype(jnp.bfloat16)
    gain_attn = (1.0 + 0.3 * jax.random.normal(weight_keys[0], (N_LAYERS, D_MODEL), jnp.float32)).astype(jnp.bfloat16)
    gain_mlp = (1.0 + 0.3 * jax.random.normal(weight_keys[1], (N_LAYERS, D_MODEL), jnp.float32)).astype(jnp.bfloat16)
    in_scale = D_MODEL ** -0.5
    key_proj = jax.random.normal(weight_keys[2], (N_LAYERS, D_MODEL, KV_HEADS, HEAD_DIM), jnp.float32) * in_scale
    query_proj = plant_gain * jnp.repeat(key_proj, GROUP_SIZE, axis=2) + jax.random.normal(weight_keys[3], (N_LAYERS, D_MODEL, N_HEADS, HEAD_DIM), jnp.float32) * in_scale
    w_query = query_proj.reshape(N_LAYERS, D_MODEL, N_HEADS * HEAD_DIM).astype(jnp.bfloat16)
    w_key = key_proj.reshape(N_LAYERS, D_MODEL, KV_HEADS * HEAD_DIM).astype(jnp.bfloat16)
    w_value = (jax.random.normal(weight_keys[4], (N_LAYERS, D_MODEL, KV_HEADS * HEAD_DIM), jnp.float32) * in_scale).astype(jnp.bfloat16)
    w_out = (jax.random.normal(weight_keys[5], (N_LAYERS, N_HEADS * HEAD_DIM, D_MODEL), jnp.float32) * (N_HEADS * HEAD_DIM) ** -0.5).astype(jnp.bfloat16)
    w_gate = (jax.random.normal(weight_keys[6], (N_LAYERS, D_MODEL, FF_DIM), jnp.float32) * in_scale).astype(jnp.bfloat16)
    w_up = (jax.random.normal(weight_keys[7], (N_LAYERS, D_MODEL, FF_DIM), jnp.float32) * in_scale).astype(jnp.bfloat16)
    w_down = (jax.random.normal(weight_keys[8], (N_LAYERS, FF_DIM, D_MODEL), jnp.float32) * FF_DIM ** -0.5).astype(jnp.bfloat16)
    return {'tok_emb': tok_emb, 'lengths': lengths, 'key_cache': key_cache, 'val_cache': val_cache, 'gain_attn': gain_attn, 'gain_mlp': gain_mlp, 'w_query': w_query, 'w_key': w_key, 'w_value': w_value, 'w_out': w_out, 'w_gate': w_gate, 'w_up': w_up, 'w_down': w_down}


def rms_norm(hidden, gain_vec):
    x_float = hidden.astype(jnp.float32)
    inv_rms = lax.rsqrt(jnp.mean(x_float * x_float, axis=-1, keepdims=True) + EPS)
    return (x_float * inv_rms * gain_vec.astype(jnp.float32)).astype(jnp.bfloat16)


def rotary(in_vecs, positions):
    head_dim = in_vecs.shape[-1]
    half_dim = head_dim // 2
    inv_freq = 1.0 / (ROPE_BASE ** (jnp.arange(half_dim).astype(jnp.float32) * 2.0 / head_dim))
    angles = positions.astype(jnp.float32)[:, None] * inv_freq[None, :]
    cos_a = jnp.cos(angles)[:, None, :]
    sin_a = jnp.sin(angles)[:, None, :]
    front_half = in_vecs[..., :half_dim]
    back_half = in_vecs[..., half_dim:]
    return jnp.concatenate([front_half * cos_a - back_half * sin_a, back_half * cos_a + front_half * sin_a], axis=-1)


def reference(tok_emb, lengths, key_cache, val_cache, gain_attn, gain_mlp, w_query, w_key, w_value, w_out, w_gate, w_up, w_down):
    slot_ids = jnp.arange(CACHE_LEN)
    slot_pos = (slot_ids % LOC_LEN) * SP_SIZE + slot_ids // LOC_LEN
    row_ids = jnp.arange(SEQ_BATCH)

    def one_step(caches, step_in):
        step_idx, hidden = step_in
        cur_pos = lengths + step_idx
        write_slot = (cur_pos % SP_SIZE) * LOC_LEN + cur_pos // SP_SIZE
        valid_mask = (slot_pos[None, :] <= cur_pos[:, None])[:, None, None, :]

        def one_layer(hidden, layer_in):
            lay_k, lay_v, gain_a, gain_m, lay_wq, lay_wk, lay_wv, lay_wo, lay_wg, lay_wu, lay_wd = layer_in
            normed = rms_norm(hidden, gain_a)
            q_vec = jnp.dot(normed, lay_wq, preferred_element_type=jnp.float32).reshape(SEQ_BATCH, N_HEADS, HEAD_DIM)
            k_vec = jnp.dot(normed, lay_wk, preferred_element_type=jnp.float32).reshape(SEQ_BATCH, KV_HEADS, HEAD_DIM)
            v_vec = jnp.dot(normed, lay_wv, preferred_element_type=jnp.float32).reshape(SEQ_BATCH, KV_HEADS, HEAD_DIM).astype(jnp.bfloat16)
            q_rot = rotary(q_vec, cur_pos).astype(jnp.bfloat16).reshape(SEQ_BATCH, KV_HEADS, GROUP_SIZE, HEAD_DIM)
            k_rot = rotary(k_vec, cur_pos).astype(jnp.bfloat16)
            lay_k = lay_k.at[row_ids, write_slot].set(k_rot)
            lay_v = lay_v.at[row_ids, write_slot].set(v_vec)
            scores = jnp.einsum('bkgd,bjkd->bkgj', q_rot.astype(jnp.float32), lay_k.astype(jnp.float32)) * HEAD_DIM ** -0.5
            scores = jnp.where(valid_mask, scores, -1e30)
            prob_w = jnp.exp(scores - jnp.max(scores, axis=-1, keepdims=True))
            denom_sum = jnp.sum(prob_w, axis=-1, keepdims=True)
            numer_sum = jnp.einsum('bkgj,bjkd->bkgd', prob_w.astype(jnp.bfloat16).astype(jnp.float32), lay_v.astype(jnp.float32))
            attn_out = (numer_sum / denom_sum).astype(jnp.bfloat16).reshape(SEQ_BATCH, N_HEADS * HEAD_DIM)
            hidden = (hidden.astype(jnp.float32) + jnp.dot(attn_out, lay_wo, preferred_element_type=jnp.float32)).astype(jnp.bfloat16)
            normed = rms_norm(hidden, gain_m)
            gate_pre = jnp.dot(normed, lay_wg, preferred_element_type=jnp.float32)
            up_pre = jnp.dot(normed, lay_wu, preferred_element_type=jnp.float32)
            mlp_act = (jax.nn.silu(gate_pre) * up_pre).astype(jnp.bfloat16)
            hidden = (hidden.astype(jnp.float32) + jnp.dot(mlp_act, lay_wd, preferred_element_type=jnp.float32)).astype(jnp.bfloat16)
            return hidden, (lay_k, lay_v)

        hidden, new_caches = lax.scan(one_layer, hidden, (caches[0], caches[1], gain_attn, gain_mlp, w_query, w_key, w_value, w_out, w_gate, w_up, w_down))
        return new_caches, hidden

    final_caches, hidden_all = lax.scan(one_step, (key_cache, val_cache), (jnp.arange(N_STEPS), tok_emb))
    return (hidden_all, final_caches[0], final_caches[1])
```

```python
import functools
import jax
import jax.numpy as jnp
from jax import lax
from jax.experimental import pallas as pl
from jax.experimental.pallas import tpu as pltpu
from jax.sharding import PartitionSpec as P

EPS = 1e-5
ROPE_BASE = 500000.0
F32 = jnp.float32
BF16 = jnp.bfloat16


def rms_norm(x_float, gain_row):
    inv_rms = lax.rsqrt(jnp.mean(x_float * x_float, axis=-1, keepdims=True) + EPS)
    return (x_float * inv_rms * gain_row).astype(BF16)


def attn_kernel(layer, n_steps, n_heads, offs_ref, u_ref, gain_ref, cos_ref, sin_ref, wq_hbm, wk_hbm, wv_hbm, kc_hbm, vc_hbm, *rest):
    if layer > 0:
        rest = rest[2:]
    o_ref, st_ref, ko_hbm, vo_hbm, wq_buf, wk_buf, wv_buf, kbuf, vbuf, q_sc, kn_sc, vn_sc, w_sem, in_sem, out_sem = rest
    n_rows = u_ref.shape[0]
    n_slots, head_dim = kbuf.shape[1], kbuf.shape[2]
    n_seq = kbuf.shape[0]
    n_pairs = n_seq // 2
    pair_rows = 2 * n_steps

    w_copies = [pltpu.make_async_copy(src.at[layer], dst, w_sem.at[i]) for i, (src, dst) in enumerate(((wq_hbm, wq_buf), (wk_hbm, wk_buf), (wv_hbm, wv_buf)))]
    for cp in w_copies:
        cp.start()

    def in_copies(i):
        sl = pl.ds(2 * i, 2)
        return (pltpu.make_async_copy(kc_hbm.at[layer, sl], kbuf.at[sl], in_sem.at[0, i]),
                pltpu.make_async_copy(vc_hbm.at[layer, sl], vbuf.at[sl], in_sem.at[1, i]))

    def out_copies(i):
        sl = pl.ds(2 * i, 2)
        return (pltpu.make_async_copy(kbuf.at[sl], ko_hbm.at[layer, sl], out_sem.at[0, i]),
                pltpu.make_async_copy(vbuf.at[sl], vo_hbm.at[layer, sl], out_sem.at[1, i]))

    @pl.loop(0, n_pairs)
    def _(i):
        for cp in in_copies(i):
            cp.start()

    h = rms_norm(u_ref[...].astype(F32), gain_ref[...].astype(F32))
    cos_t = cos_ref[...]
    sin_t = sin_ref[...]

    def rope(x):
        return (x * cos_t + pltpu.roll(x, head_dim // 2, 1) * sin_t).astype(BF16).astype(F32)

    for cp in w_copies:
        cp.wait()
    q_all = jnp.dot(h, wq_buf[...], preferred_element_type=F32)
    for hd in range(n_heads):
        q_sc[hd] = rope(q_all[:, hd * head_dim:(hd + 1) * head_dim])
    kn_sc[...] = rope(jnp.dot(h, wk_buf[...], preferred_element_type=F32))
    vn_sc[...] = jnp.dot(h, wv_buf[...], preferred_element_type=F32).astype(BF16).astype(F32)

    m_rows = n_heads * pair_rows
    scale = head_dim ** -0.5

    def pair_body(i):
        for cp in in_copies(i):
            cp.wait()
        sub = lax.broadcasted_iota(jnp.int32, (m_rows, 1), 0) % pair_rows
        first = sub < n_steps
        q48 = jnp.concatenate([q_sc[hd, pl.ds(pair_rows * i, pair_rows), :] for hd in range(n_heads)], axis=0).astype(BF16)
        scs = []
        for e in range(2):
            b = 2 * i + e
            off = offs_ref[0, b]
            slot = offs_ref[1, b]
            row = offs_ref[2, b]
            base = pl.multiple_of((slot // 16) * 16, 16)
            hit = lax.broadcasted_iota(jnp.int32, (16, head_dim), 0) == slot - base
            for buf, new in ((kbuf, kn_sc), (vbuf, vn_sc)):
                tile = buf[b, pl.ds(base, 16), :].astype(F32)
                new_row = new[pl.ds(row, 1), :]
                buf[b, pl.ds(base, 16), :] = jnp.where(hit, jnp.broadcast_to(new_row, (16, head_dim)), tile).astype(BF16)
            scs.append(lax.dot_general(q48, kbuf[b], (((1,), (1,)), ((), ())), preferred_element_type=F32))
        lim = (jnp.where(first, offs_ref[0, 2 * i] + sub, offs_ref[0, 2 * i + 1] + sub - n_steps)) // 4
        s = jnp.where(jnp.broadcast_to(first, scs[0].shape), scs[0], scs[1]) * scale
        slot_id = lax.broadcasted_iota(jnp.int32, s.shape, 1)
        s = jnp.where(slot_id <= lim, s, -1e30)
        m = jnp.max(s, axis=-1, keepdims=True)
        p = jnp.exp(s - m)
        l = jnp.sum(p, axis=-1, keepdims=True)
        pb = p.astype(BF16)
        o0 = jnp.dot(pb, vbuf[2 * i], preferred_element_type=F32)
        o1 = jnp.dot(pb, vbuf[2 * i + 1], preferred_element_type=F32)
        o = jnp.where(jnp.broadcast_to(first, o0.shape), o0, o1)
        lane = lax.broadcasted_iota(jnp.int32, (pair_rows, head_dim), 1)
        st = jnp.zeros((pair_rows, head_dim), F32)
        for hd in range(n_heads):
            rs = slice(hd * pair_rows, (hd + 1) * pair_rows)
            o_ref[hd, pl.ds(pair_rows * i, pair_rows), :] = o[rs]
            st = jnp.where(lane == hd, m[rs], jnp.where(lane == hd + 8, l[rs], st))
        st_ref[pl.ds(pair_rows * i, pair_rows), :] = st
        for cp in out_copies(i):
            cp.start()

    @pl.loop(0, n_pairs // 2)
    def _(i):
        pair_body(2 * i)
        pair_body(2 * i + 1)

    @pl.loop(0, n_pairs)
    def _(i):
        for cp in out_copies(i):
            cp.wait()


def attention(layer, n_steps, offs, u, gain, cos_t, sin_t, w_query, w_key, w_value, kc, vc, prev):
    n_layers, n_seq, n_slots, head_dim = kc.shape
    n_rows, d_model = u.shape
    q_cols = w_query.shape[2]
    n_heads = q_cols // head_dim
    any_spec = pl.BlockSpec(memory_space=pl.ANY)
    vm = pl.BlockSpec(memory_space=pltpu.VMEM)
    ins = [offs, u, gain, cos_t, sin_t, w_query, w_key, w_value, kc, vc]
    in_specs = [pl.BlockSpec(memory_space=pltpu.SMEM), vm, vm, vm, vm] + [any_spec] * 5
    aliases = {}
    if layer > 0:
        ins += list(prev)
        in_specs += [any_spec] * 2
        aliases = {10: 2, 11: 3}
    cache_t = jax.ShapeDtypeStruct(kc.shape, kc.dtype)
    return pl.pallas_call(
        functools.partial(attn_kernel, layer, n_steps, n_heads),
        out_shape=[jax.ShapeDtypeStruct((n_heads, n_rows, head_dim), F32), jax.ShapeDtypeStruct((n_rows, head_dim), F32), cache_t, cache_t],
        in_specs=in_specs,
        out_specs=[vm, vm, any_spec, any_spec],
        scratch_shapes=[
            pltpu.VMEM((d_model, q_cols), BF16), pltpu.VMEM((d_model, head_dim), BF16), pltpu.VMEM((d_model, head_dim), BF16),
            pltpu.VMEM((n_seq, n_slots, head_dim), BF16), pltpu.VMEM((n_seq, n_slots, head_dim), BF16),
            pltpu.VMEM((n_heads, n_rows, head_dim), F32), pltpu.VMEM((n_rows, head_dim), F32), pltpu.VMEM((n_rows, head_dim), F32),
            pltpu.SemaphoreType.DMA((3,)), pltpu.SemaphoreType.DMA((2, n_seq // 2)), pltpu.SemaphoreType.DMA((2, n_seq // 2)),
        ],
        input_output_aliases=aliases,
        compiler_params=pltpu.CompilerParams(vmem_limit_bytes=40 * 1024 * 1024),
        name=f"attn{layer}",
    )(*ins)


def solution(mesh):
    sp_size = mesh.shape['sp']

    def local_fn(tok_emb, lengths, key_cache, val_cache, gain_attn, gain_mlp, w_query, w_key, w_value, w_out, w_gate, w_up, w_down):
        n_steps, n_batch, d_model = tok_emb.shape
        n_layers, _, loc_len, kv_loc, head_dim = key_cache.shape
        n_heads = w_query.shape[2] // head_dim
        n_rows = n_steps * n_batch
        my_sp = lax.axis_index('sp')
        kc = key_cache.reshape(n_layers, n_batch, loc_len, head_dim)
        vc = val_cache.reshape(n_layers, n_batch, loc_len, head_dim)
        own_step = (my_sp - lengths) % sp_size
        offs = jnp.stack([lengths - my_sp, (lengths + own_step) // sp_size, jnp.arange(n_batch, dtype=jnp.int32) * n_steps + own_step]).astype(jnp.int32)
        positions = (lengths[:, None] + jnp.arange(n_steps)[None, :]).reshape(n_rows)
        half_dim = head_dim // 2
        inv_freq = 1.0 / (ROPE_BASE ** (jnp.arange(half_dim).astype(F32) * 2.0 / head_dim))
        angles = positions.astype(F32)[:, None] * inv_freq[None, :]
        cos_a, sin_a = jnp.cos(angles), jnp.sin(angles)
        cos_t = jnp.concatenate([cos_a, cos_a], axis=-1)
        sin_t = jnp.concatenate([-sin_a, sin_a], axis=-1)
        u = tok_emb.transpose(1, 0, 2).reshape(n_rows, d_model)
        prev = None
        for layer in range(n_layers):
            o, st, ko, vo = attention(layer, n_steps, offs, u, gain_attn[layer][None], cos_t, sin_t, w_query, w_key, w_value, kc, vc, prev)
            prev = (ko, vo)
            loc_max = st[:, :n_heads].T[..., None]
            loc_sum = st[:, 8:8 + n_heads].T[..., None]
            glob_max = lax.pmax(loc_max, 'sp')
            merged = lax.psum(jnp.concatenate([o, loc_sum], axis=-1) * jnp.exp(loc_max - glob_max), 'sp')
            attn_out = (merged[..., :head_dim] / merged[..., head_dim:]).astype(BF16).transpose(1, 0, 2).reshape(n_rows, n_heads * head_dim)
            proj = lax.psum(jnp.dot(attn_out, w_out[layer], preferred_element_type=F32), 'tp')
            u = (u.astype(F32) + proj).astype(BF16)
            h2 = rms_norm(u.astype(F32), gain_mlp[layer].astype(F32))
            act = (jax.nn.silu(jnp.dot(h2, w_gate[layer], preferred_element_type=F32)) * jnp.dot(h2, w_up[layer], preferred_element_type=F32)).astype(BF16)
            down = lax.psum(jnp.dot(act, w_down[layer], preferred_element_type=F32), 'tp')
            u = (u.astype(F32) + down).astype(BF16)
        hidden = u.reshape(n_batch, n_steps, d_model).transpose(1, 0, 2)
        return hidden, prev[0].reshape(key_cache.shape), prev[1].reshape(val_cache.shape)

    cache_spec = P(None, 'dp', 'sp', 'tp', None)
    col_spec = P(None, None, 'tp')
    row_spec = P(None, 'tp', None)
    emb_spec = P(None, 'dp', None)
    return jax.shard_map(local_fn, mesh=mesh, in_specs=(emb_spec, P('dp'), cache_spec, cache_spec, P(), P(), col_spec, col_spec, col_spec, row_spec, col_spec, col_spec, row_spec), out_specs=(emb_spec, cache_spec, cache_spec), check_vma=False)
```

```python
import functools
import jax
import jax.numpy as jnp
from jax import lax
from jax.experimental import pallas as pl
from jax.experimental.pallas import tpu as pltpu
from jax.sharding import PartitionSpec as P

EPS = 1e-5
ROPE_BASE = 500000.0
F32 = jnp.float32
BF16 = jnp.bfloat16
MESH = pl.DeviceIdType.MESH


def rms_norm(x_float, gain_row):
    inv_rms = lax.rsqrt(jnp.mean(x_float * x_float, axis=-1, keepdims=True) + EPS)
    return (x_float * inv_rms * gain_row).astype(BF16)


def attn_kernel(layer, n_steps, n_heads, offs_ref, u_ref, gain_ref, cos_ref, sin_ref, wq_hbm, wk_hbm, wv_hbm, kc_hbm, vc_hbm, *rest):
    if layer > 0:
        rest = rest[2:]
    o_ref, ko_hbm, vo_hbm, wq_buf, wk_buf, wv_buf, kbuf, vbuf, q_sc, kn_sc, vn_sc, w_sem, in_sem, out_sem = rest
    n_rows = u_ref.shape[0]
    n_slots, head_dim = kbuf.shape[1], kbuf.shape[2]
    n_seq = kbuf.shape[0]
    n_pairs = n_seq // 2
    pair_rows = 2 * n_steps

    w_copies = [pltpu.make_async_copy(src.at[layer], dst, w_sem.at[i]) for i, (src, dst) in enumerate(((wq_hbm, wq_buf), (wk_hbm, wk_buf), (wv_hbm, wv_buf)))]
    for cp in w_copies:
        cp.start()

    def in_copies(i):
        sl = pl.ds(2 * i, 2)
        return (pltpu.make_async_copy(kc_hbm.at[layer, sl], kbuf.at[sl], in_sem.at[0, i]),
                pltpu.make_async_copy(vc_hbm.at[layer, sl], vbuf.at[sl], in_sem.at[1, i]))

    def out_copies(i):
        sl = pl.ds(2 * i, 2)
        return (pltpu.make_async_copy(kbuf.at[sl], ko_hbm.at[layer, sl], out_sem.at[0, i]),
                pltpu.make_async_copy(vbuf.at[sl], vo_hbm.at[layer, sl], out_sem.at[1, i]))

    @pl.loop(0, n_pairs)
    def _(i):
        for cp in in_copies(i):
            cp.start()

    h = rms_norm(u_ref[...].astype(F32), gain_ref[...].astype(F32))
    cos_t = cos_ref[...]
    sin_t = sin_ref[...]

    def rope(x):
        return (x * cos_t + pltpu.roll(x, head_dim // 2, 1) * sin_t).astype(BF16).astype(F32)

    for cp in w_copies:
        cp.wait()
    q_all = jnp.dot(h, wq_buf[...], preferred_element_type=F32)
    for hd in range(n_heads):
        q_sc[hd] = rope(q_all[:, hd * head_dim:(hd + 1) * head_dim])
    kn_sc[...] = rope(jnp.dot(h, wk_buf[...], preferred_element_type=F32))
    vn_sc[...] = jnp.dot(h, wv_buf[...], preferred_element_type=F32).astype(BF16).astype(F32)

    m_rows = n_heads * pair_rows
    scale = head_dim ** -0.5

    def pair_body(i):
        for cp in in_copies(i):
            cp.wait()
        sub = lax.broadcasted_iota(jnp.int32, (m_rows, 1), 0) % pair_rows
        first = sub < n_steps
        q48 = jnp.concatenate([q_sc[hd, pl.ds(pair_rows * i, pair_rows), :] for hd in range(n_heads)], axis=0).astype(BF16)
        scs = []
        for e in range(2):
            b = 2 * i + e
            off = offs_ref[0, b]
            slot = offs_ref[1, b]
            row = offs_ref[2, b]
            base = pl.multiple_of((slot // 16) * 16, 16)
            hit = lax.broadcasted_iota(jnp.int32, (16, head_dim), 0) == slot - base
            for buf, new in ((kbuf, kn_sc), (vbuf, vn_sc)):
                tile = buf[b, pl.ds(base, 16), :].astype(F32)
                new_row = new[pl.ds(row, 1), :]
                buf[b, pl.ds(base, 16), :] = jnp.where(hit, jnp.broadcast_to(new_row, (16, head_dim)), tile).astype(BF16)
            scs.append(lax.dot_general(q48, kbuf[b], (((1,), (1,)), ((), ())), preferred_element_type=F32))
        lim = (jnp.where(first, offs_ref[0, 2 * i] + sub, offs_ref[0, 2 * i + 1] + sub - n_steps)) // 4
        s = jnp.where(jnp.broadcast_to(first, scs[0].shape), scs[0], scs[1]) * scale
        slot_id = lax.broadcasted_iota(jnp.int32, s.shape, 1)
        s = jnp.where(slot_id <= lim, s, -1e30)
        m = jnp.max(s, axis=-1, keepdims=True)
        p = jnp.exp(s - m)
        l = jnp.sum(p, axis=-1, keepdims=True)
        pb = p.astype(BF16)
        o0 = jnp.dot(pb, vbuf[2 * i], preferred_element_type=F32)
        o1 = jnp.dot(pb, vbuf[2 * i + 1], preferred_element_type=F32)
        o = jnp.where(jnp.broadcast_to(first, o0.shape), o0, o1)
        lane = lax.broadcasted_iota(jnp.int32, (pair_rows, head_dim), 1)
        st = jnp.zeros((pair_rows, head_dim), F32)
        for hd in range(n_heads):
            rs = slice(hd * pair_rows, (hd + 1) * pair_rows)
            o_ref[hd, pl.ds(pair_rows * i, pair_rows), :] = o[rs]
            st = jnp.where(lane == hd, m[rs], jnp.where(lane == hd + 8, l[rs], st))
        o_ref[n_heads, pl.ds(pair_rows * i, pair_rows), :] = st
        for cp in out_copies(i):
            cp.start()

    @pl.loop(0, n_pairs // 2)
    def _(i):
        pair_body(2 * i)
        pair_body(2 * i + 1)

    @pl.loop(0, n_pairs)
    def _(i):
        for cp in out_copies(i):
            cp.wait()


def attention(layer, n_steps, offs, u, gain, cos_t, sin_t, w_query, w_key, w_value, kc, vc, prev):
    n_layers, n_seq, n_slots, head_dim = kc.shape
    n_rows, d_model = u.shape
    q_cols = w_query.shape[2]
    n_heads = q_cols // head_dim
    any_spec = pl.BlockSpec(memory_space=pl.ANY)
    vm = pl.BlockSpec(memory_space=pltpu.VMEM)
    ins = [offs, u, gain, cos_t, sin_t, w_query, w_key, w_value, kc, vc]
    in_specs = [pl.BlockSpec(memory_space=pltpu.SMEM), vm, vm, vm, vm] + [any_spec] * 5
    aliases = {}
    if layer > 0:
        ins += list(prev)
        in_specs += [any_spec] * 2
        aliases = {10: 1, 11: 2}
    cache_t = jax.ShapeDtypeStruct(kc.shape, kc.dtype)
    return pl.pallas_call(
        functools.partial(attn_kernel, layer, n_steps, n_heads),
        out_shape=[jax.ShapeDtypeStruct((n_heads + 1, n_rows, head_dim), F32), cache_t, cache_t],
        in_specs=in_specs,
        out_specs=[vm, any_spec, any_spec],
        scratch_shapes=[
            pltpu.VMEM((d_model, q_cols), BF16), pltpu.VMEM((d_model, head_dim), BF16), pltpu.VMEM((d_model, head_dim), BF16),
            pltpu.VMEM((n_seq, n_slots, head_dim), BF16), pltpu.VMEM((n_seq, n_slots, head_dim), BF16),
            pltpu.VMEM((n_heads, n_rows, head_dim), F32), pltpu.VMEM((n_rows, head_dim), F32), pltpu.VMEM((n_rows, head_dim), F32),
            pltpu.SemaphoreType.DMA((3,)), pltpu.SemaphoreType.DMA((2, n_seq // 2)), pltpu.SemaphoreType.DMA((2, n_seq // 2)),
        ],
        input_output_aliases=aliases,
        compiler_params=pltpu.CompilerParams(vmem_limit_bytes=40 * 1024 * 1024),
        name=f"attn{layer}",
    )(*ins)


def merge(a, b, n_heads):
    lane = lax.broadcasted_iota(jnp.int32, a(n_heads).shape, 1)
    st_a, st_b = a(n_heads), b(n_heads)
    m = jnp.maximum(st_a, st_b)
    fa, fb = jnp.exp(st_a - m), jnp.exp(st_b - m)
    fa = jnp.where(lane < 8, fa, 0.0)
    fb = jnp.where(lane < 8, fb, 0.0)
    l = st_a * pltpu.roll(fa, 8, 1) + st_b * pltpu.roll(fb, 8, 1)
    st = jnp.where(lane < 8, m, l)
    outs = [a(hd) * fa[:, hd:hd + 1] + b(hd) * fb[:, hd:hd + 1] for hd in range(n_heads)]
    return outs, st


def mix_kernel(layer, n_heads, part_ref, u_ref, gain_ref, wo_hbm, wg_hbm, wu_hbm, wd_hbm, out_ref,
               wo_buf, wg_buf, wu_buf, wd_buf, core_in, fwd_out, fwd_in, y_out, y_in, u1_sc, h_out, h_in, hh, act,
               d_own, d_out, d_in, e_out, e_in, u_all, w_sem, send_sem, recv_sem):
    tp = lax.axis_index('tp')
    sp = lax.axis_index('sp')
    core = lax.rem(sp, 2)
    core_peer = {'sp': sp + 1 - 2 * core}
    far_peer = {'sp': lax.rem(sp + 2, 4)}
    tp_peer = {'tp': 1 - tp}
    n_blk, chunk, width = y_out.shape
    ff = wg_buf.shape[1]
    skip = 2 * ff - wg_hbm.shape[2]
    col0 = pl.multiple_of(core * (ff - skip), 128)

    w_copies = [
        pltpu.make_async_copy(wo_hbm.at[layer], wo_buf, w_sem.at[0]),
        pltpu.make_async_copy(wg_hbm.at[layer, :, pl.ds(col0, ff)], wg_buf, w_sem.at[1]),
        pltpu.make_async_copy(wu_hbm.at[layer, :, pl.ds(col0, ff)], wu_buf, w_sem.at[2]),
        pltpu.make_async_copy(wd_hbm.at[layer, pl.ds(col0, ff), :], wd_buf, w_sem.at[3]),
    ]
    for cp in w_copies:
        cp.start()

    barrier = pltpu.get_barrier_semaphore()
    for peer in (core_peer, far_peer, tp_peer):
        pl.semaphore_signal(barrier, inc=1, device_id=peer, device_id_type=MESH)
    pl.semaphore_wait(barrier, 3)

    count = [0]

    def remote(src, dst, peer):
        k = count[0]
        count[0] += 1
        return pltpu.make_async_remote_copy(src_ref=src, dst_ref=dst, send_sem=send_sem.at[k], recv_sem=recv_sem.at[k], device_id=peer, device_id_type=MESH)

    def rows(idx):
        return pl.ds(pl.multiple_of(idx * chunk, chunk), chunk)

    far_chunk = lax.rem(sp + 2, 4)
    sib = sp + 1 - 2 * core
    sib_far = lax.rem(sib + 2, 4)

    c_far = remote(part_ref.at[:, rows(sib_far), :], core_in.at[0], core_peer)
    c_own = remote(part_ref.at[:, rows(sib), :], core_in.at[1], core_peer)
    c_far.start()
    c_own.start()
    fwd = remote(fwd_out, fwd_in, far_peer)
    c_far.wait_recv()
    outs, st = merge(lambda hd: part_ref[hd, rows(far_chunk), :], lambda hd: core_in[0, hd], n_heads)
    for hd in range(n_heads):
        fwd_out[hd] = outs[hd]
    fwd_out[n_heads] = st
    fwd.start()
    c_own.wait_recv()
    own, own_st = merge(lambda hd: part_ref[hd, rows(sp), :], lambda hd: core_in[1, hd], n_heads)
    for hd in range(n_heads):
        core_in[0, hd] = own[hd]
    core_in[0, n_heads] = own_st
    fwd.wait_recv()
    outs, st = merge(lambda hd: core_in[0, hd], lambda hd: fwd_in[hd], n_heads)
    attn_out = jnp.concatenate([(outs[hd] / st[:, 8 + hd:9 + hd]).astype(BF16) for hd in range(n_heads)], axis=1)

    y_copies = [remote(y_out.at[n], y_in.at[n], tp_peer) for n in range(n_blk)]
    w_copies[0].wait()
    for n in range(n_blk):
        y_out[n] = jnp.dot(attn_out, wo_buf[:, n * width:(n + 1) * width], preferred_element_type=F32)
        y_copies[n].start()
    for n in range(n_blk):
        y_copies[n].wait_recv()
        cols = slice(n * width, (n + 1) * width)
        u1_sc[:, cols] = (u_ref[rows(sp), cols].astype(F32) + (y_out[n] + y_in[n])).astype(BF16).astype(F32)
    h2 = rms_norm(u1_sc[...], gain_ref[...].astype(F32))
    h_out[...] = h2.astype(F32)
    hh[0:chunk, :] = h2
    h_copy = remote(h_out, h_in, core_peer)
    h_copy.start()
    for cp in w_copies[1:]:
        cp.wait()
    h_copy.wait_recv()
    hh[chunk:2 * chunk, :] = h_in[...].astype(BF16)

    blk = 256
    for n in range(ff // blk):
        cols = slice(n * blk, (n + 1) * blk)
        gate = jnp.dot(hh[...], wg_buf[:, cols], preferred_element_type=F32)
        up = jnp.dot(hh[...], wu_buf[:, cols], preferred_element_type=F32)
        val = gate / (1.0 + jnp.exp(-gate)) * up
        if n * blk < skip:
            lane = lax.broadcasted_iota(jnp.int32, val.shape, 1) + n * blk
            val = jnp.where(lane < skip * core, 0.0, val)
        act[:, cols] = val.astype(BF16)

    d_copies = [remote(d_out.at[n], d_in.at[n], core_peer) for n in range(n_blk)]
    e_copies = [remote(e_out.at[n], e_in.at[n], tp_peer) for n in range(n_blk)]
    a_core = [remote(u_all.at[n, rows(sp), :], u_all.at[n, rows(sp), :], core_peer) for n in range(n_blk)]
    a_far = [remote(u_all.at[n, rows(sp), :], u_all.at[n, rows(sp), :], far_peer) for n in range(n_blk)]
    a_fwd = [remote(u_all.at[n, rows(far_chunk), :], u_all.at[n, rows(far_chunk), :], core_peer) for n in range(n_blk)]
    for n in range(n_blk):
        down = jnp.dot(act[...], wd_buf[:, n * width:(n + 1) * width], preferred_element_type=F32)
        d_own[n] = down[:chunk]
        d_out[n] = down[chunk:]
        d_copies[n].start()
    for n in range(n_blk):
        d_copies[n].wait_recv()
        e_out[n] = d_own[n] + d_in[n]
        e_copies[n].start()
    for n in range(n_blk):
        e_copies[n].wait_recv()
        u_all[n, rows(sp), :] = (u1_sc[:, n * width:(n + 1) * width] + (e_out[n] + e_in[n])).astype(BF16).astype(F32)
        a_far[n].start()
        a_core[n].start()
    for n in range(n_blk):
        a_far[n].wait_recv()
        a_fwd[n].start()
    for n in range(n_blk):
        a_core[n].wait_recv()
        a_fwd[n].wait_recv()
        out_ref[:, n * width:(n + 1) * width] = u_all[n].astype(BF16)
    for cp in [c_far, c_own, fwd, h_copy] + y_copies + d_copies + e_copies + a_core + a_far + a_fwd:
        cp.wait_send()


def mix(layer, part, u, gain, w_out, w_gate, w_up, w_down):
    n_planes, n_rows, head_dim = part.shape
    n_heads = n_planes - 1
    d_model = u.shape[1]
    chunk = n_rows // 4
    n_tiles = w_gate.shape[2] // 128
    ff = ((n_tiles + 1) // 2) * 128
    n_blk = 3
    width = d_model // n_blk
    any_spec = pl.BlockSpec(memory_space=pl.ANY)
    vm = pl.BlockSpec(memory_space=pltpu.VMEM)
    blocks = pltpu.VMEM((n_blk, chunk, width), F32)
    planes = pltpu.VMEM((n_planes, chunk, head_dim), F32)
    n_copies = 4 + 6 * n_blk
    return pl.pallas_call(
        functools.partial(mix_kernel, layer, n_heads),
        out_shape=jax.ShapeDtypeStruct((n_rows, d_model), BF16),
        in_specs=[vm, vm, vm] + [any_spec] * 4,
        out_specs=vm,
        scratch_shapes=[
            pltpu.VMEM((w_out.shape[1], d_model), BF16), pltpu.VMEM((d_model, ff), BF16), pltpu.VMEM((d_model, ff), BF16), pltpu.VMEM((ff, d_model), BF16),
            pltpu.VMEM((2, n_planes, chunk, head_dim), F32), planes, planes,
            blocks, blocks, pltpu.VMEM((chunk, d_model), F32), pltpu.VMEM((chunk, d_model), F32), pltpu.VMEM((chunk, d_model), F32),
            pltpu.VMEM((2 * chunk, d_model), BF16), pltpu.VMEM((2 * chunk, ff), BF16),
            blocks, blocks, blocks, blocks, blocks, pltpu.VMEM((n_blk, n_rows, width), F32),
            pltpu.SemaphoreType.DMA((4,)), pltpu.SemaphoreType.DMA((n_copies,)), pltpu.SemaphoreType.DMA((n_copies,)),
        ],
        compiler_params=pltpu.CompilerParams(collective_id=layer, has_side_effects=True, vmem_limit_bytes=48 * 1024 * 1024),
        name=f"mix{layer}",
    )(part, u, gain, w_out, w_gate, w_up, w_down)


def solution(mesh):
    sp_size = mesh.shape['sp']

    def local_fn(tok_emb, lengths, key_cache, val_cache, gain_attn, gain_mlp, w_query, w_key, w_value, w_out, w_gate, w_up, w_down):
        n_steps, n_batch, d_model = tok_emb.shape
        n_layers, _, loc_len, kv_loc, head_dim = key_cache.shape
        n_heads = w_query.shape[2] // head_dim
        n_rows = n_steps * n_batch
        my_sp = lax.axis_index('sp')
        kc = key_cache.reshape(n_layers, n_batch, loc_len, head_dim)
        vc = val_cache.reshape(n_layers, n_batch, loc_len, head_dim)
        own_step = (my_sp - lengths) % sp_size
        offs = jnp.stack([lengths - my_sp, (lengths + own_step) // sp_size, jnp.arange(n_batch, dtype=jnp.int32) * n_steps + own_step]).astype(jnp.int32)
        positions = (lengths[:, None] + jnp.arange(n_steps)[None, :]).reshape(n_rows)
        half_dim = head_dim // 2
        inv_freq = 1.0 / (ROPE_BASE ** (jnp.arange(half_dim).astype(F32) * 2.0 / head_dim))
        angles = positions.astype(F32)[:, None] * inv_freq[None, :]
        cos_a, sin_a = jnp.cos(angles), jnp.sin(angles)
        cos_t = jnp.concatenate([cos_a, cos_a], axis=-1)
        sin_t = jnp.concatenate([-sin_a, sin_a], axis=-1)
        u = tok_emb.transpose(1, 0, 2).reshape(n_rows, d_model)
        prev = None
        for layer in range(n_layers):
            part, ko, vo = attention(layer, n_steps, offs, u, gain_attn[layer][None], cos_t, sin_t, w_query, w_key, w_value, kc, vc, prev)
            prev = (ko, vo)
            u = mix(layer, part, u, gain_mlp[layer][None], w_out, w_gate, w_up, w_down)
        hidden = u.reshape(n_batch, n_steps, d_model).transpose(1, 0, 2)
        return hidden, prev[0].reshape(key_cache.shape), prev[1].reshape(val_cache.shape)

    cache_spec = P(None, 'dp', 'sp', 'tp', None)
    col_spec = P(None, None, 'tp')
    row_spec = P(None, 'tp', None)
    emb_spec = P(None, 'dp', None)
    return jax.shard_map(local_fn, mesh=mesh, in_specs=(emb_spec, P('dp'), cache_spec, cache_spec, P(), P(), col_spec, col_spec, col_spec, row_spec, col_spec, col_spec, row_spec), out_specs=(emb_spec, cache_spec, cache_spec), check_vma=False)
```

```python
import functools
import jax
import jax.numpy as jnp
import numpy as np
from jax import lax
from jax.experimental import pallas as pl
from jax.experimental.pallas import tpu as pltpu
from jax.sharding import PartitionSpec as P

EPS = 1e-5
ROPE_BASE = 500000.0
F32 = jnp.float32
BF16 = jnp.bfloat16
MESH = pl.DeviceIdType.MESH
ATTN_VMEM = 40 * 1024 * 1024
MIX_VMEM = 48 * 1024 * 1024


def rms_norm(x_float, gain_row):
    inv_rms = lax.rsqrt(jnp.mean(x_float * x_float, axis=-1, keepdims=True) + EPS)
    return (x_float * inv_rms * gain_row).astype(BF16)


def attn_kernel(layer, n_steps, n_heads, len_hbm, u_in, gain_hbm, freq_hbm, wq_hbm, wk_hbm, wv_hbm, kc_hbm, vc_hbm, *rest):
    if layer > 0:
        rest = rest[2:]
        o_ref, ko_hbm, vo_hbm = rest[:3]
    else:
        o_ref, ko_hbm, vo_hbm, u_perm = rest[:4]
        rest = rest[1:]
    wq_buf, wk_buf, wv_buf, kbuf, vbuf, q_sc, kn_sc, vn_sc, len_ref, gain_ref, freq_ref, u_buf, w_sem, in_sem, out_sem = rest[3:]
    sp = lax.axis_index('sp')
    n_rows = u_in.shape[0]
    n_slots, head_dim = kbuf.shape[1], kbuf.shape[2]
    n_seq = kbuf.shape[0]
    n_pairs = n_seq // 2
    pair_rows = 2 * n_steps

    w_copies = [pltpu.make_async_copy(src.at[layer], dst, w_sem.at[i]) for i, (src, dst) in enumerate(((wq_hbm, wq_buf), (wk_hbm, wk_buf), (wv_hbm, wv_buf)))]
    smalls = [(len_hbm, len_ref), (gain_hbm, gain_ref), (freq_hbm, freq_ref)] + ([(u_in, u_buf)] if layer == 0 else [])
    smalls = [pltpu.make_async_copy(src, dst, w_sem.at[3 + i]) for i, (src, dst) in enumerate(smalls)]
    for cp in smalls + w_copies:
        cp.start()

    def in_copies(i):
        sl = pl.ds(2 * i, 2)
        return (pltpu.make_async_copy(kc_hbm.at[layer, sl], kbuf.at[sl], in_sem.at[0, i]),
                pltpu.make_async_copy(vc_hbm.at[layer, sl], vbuf.at[sl], in_sem.at[1, i]))

    def out_copies(i):
        sl = pl.ds(2 * i, 2)
        return (pltpu.make_async_copy(kbuf.at[sl], ko_hbm.at[layer, sl], out_sem.at[0, i]),
                pltpu.make_async_copy(vbuf.at[sl], vo_hbm.at[layer, sl], out_sem.at[1, i]))

    @pl.loop(0, n_pairs)
    def _(i):
        for cp in in_copies(i):
            cp.start()

    for cp in smalls:
        cp.wait()
    if layer == 0:
        row = lax.broadcasted_iota(jnp.int32, (n_rows, n_rows), 0)
        col = lax.broadcasted_iota(jnp.int32, (n_rows, n_rows), 1)
        perm = jnp.where(col == (row % n_steps) * n_seq + row // n_steps, 1.0, 0.0).astype(BF16)
        u = jnp.dot(perm, u_buf[...], preferred_element_type=F32)
        u_perm[...] = u.astype(BF16)
    else:
        u = u_in[...].astype(F32)
    h = rms_norm(u, gain_ref[layer:layer + 1, :].astype(F32))
    sub8 = lax.broadcasted_iota(jnp.int32, (pair_rows, head_dim), 0)
    pos = jnp.concatenate([jnp.where(sub8 < n_steps, len_ref[2 * i], len_ref[2 * i + 1]) + sub8 % n_steps for i in range(n_pairs)], axis=0)
    angles = pos.astype(F32) * freq_ref[...]
    lane = lax.broadcasted_iota(jnp.int32, angles.shape, 1)
    cos_t = jnp.cos(angles)
    sin_t = jnp.sin(angles)
    sin_t = jnp.where(lane < head_dim // 2, -sin_t, sin_t)

    def rope(x):
        return (x * cos_t + pltpu.roll(x, head_dim // 2, 1) * sin_t).astype(BF16).astype(F32)

    for cp in w_copies:
        cp.wait()
    q_all = jnp.dot(h, wq_buf[...], preferred_element_type=F32)
    for hd in range(n_heads):
        q_sc[hd] = rope(q_all[:, hd * head_dim:(hd + 1) * head_dim])
    kn_sc[...] = rope(jnp.dot(h, wk_buf[...], preferred_element_type=F32))
    vn_sc[...] = jnp.dot(h, wv_buf[...], preferred_element_type=F32).astype(BF16).astype(F32)

    m_rows = n_heads * pair_rows
    scale = head_dim ** -0.5

    def pair_body(i):
        for cp in in_copies(i):
            cp.wait()
        sub = lax.broadcasted_iota(jnp.int32, (m_rows, 1), 0) % pair_rows
        first = sub < n_steps
        q48 = jnp.concatenate([q_sc[hd, pl.ds(pair_rows * i, pair_rows), :] for hd in range(n_heads)], axis=0).astype(BF16)
        scs = []
        for e in range(2):
            b = 2 * i + e
            step = (len_ref[b] + (4 - sp)) & 3
            step = (4 - step) & 3
            slot = (len_ref[b] + step) // 4
            row = n_steps * b + step
            base = pl.multiple_of((slot // 16) * 16, 16)
            hit = lax.broadcasted_iota(jnp.int32, (16, head_dim), 0) == slot - base
            for buf, new in ((kbuf, kn_sc), (vbuf, vn_sc)):
                tile = buf[b, pl.ds(base, 16), :].astype(F32)
                new_row = new[pl.ds(row, 1), :]
                buf[b, pl.ds(base, 16), :] = jnp.where(hit, jnp.broadcast_to(new_row, (16, head_dim)), tile).astype(BF16)
            scs.append(lax.dot_general(q48, kbuf[b], (((1,), (1,)), ((), ())), preferred_element_type=F32))
        lim = (jnp.where(first, len_ref[2 * i] + sub, len_ref[2 * i + 1] + sub - n_steps) - sp) // 4
        s = jnp.where(jnp.broadcast_to(first, scs[0].shape), scs[0], scs[1]) * scale
        slot_id = lax.broadcasted_iota(jnp.int32, s.shape, 1)
        s = jnp.where(slot_id <= lim, s, -1e30)
        m = jnp.max(s, axis=-1, keepdims=True)
        p = jnp.exp(s - m)
        l = jnp.sum(p, axis=-1, keepdims=True)
        pb = p.astype(BF16)
        o0 = jnp.dot(pb, vbuf[2 * i], preferred_element_type=F32)
        o1 = jnp.dot(pb, vbuf[2 * i + 1], preferred_element_type=F32)
        o = jnp.where(jnp.broadcast_to(first, o0.shape), o0, o1)
        lane = lax.broadcasted_iota(jnp.int32, (pair_rows, head_dim), 1)
        st = jnp.zeros((pair_rows, head_dim), F32)
        for hd in range(n_heads):
            rs = slice(hd * pair_rows, (hd + 1) * pair_rows)
            o_ref[hd, pl.ds(pair_rows * i, pair_rows), :] = o[rs]
            st = jnp.where(lane == hd, m[rs], jnp.where(lane == hd + 8, l[rs], st))
        o_ref[n_heads, pl.ds(pair_rows * i, pair_rows), :] = st
        for cp in out_copies(i):
            cp.start()

    @pl.loop(0, n_pairs // 2)
    def _(i):
        pair_body(2 * i)
        pair_body(2 * i + 1)

    @pl.loop(0, n_pairs)
    def _(i):
        for cp in out_copies(i):
            cp.wait()


def attention(layer, n_steps, lengths, u, gain, freq, w_query, w_key, w_value, kc, vc, prev):
    n_layers, n_seq, n_slots, head_dim = kc.shape
    n_rows, d_model = u.shape
    q_cols = w_query.shape[2]
    n_heads = q_cols // head_dim
    any_spec = pl.BlockSpec(memory_space=pltpu.HBM)
    vm = pl.BlockSpec(memory_space=pltpu.VMEM)
    ins = [lengths, u, gain, freq, w_query, w_key, w_value, kc, vc]
    in_specs = [any_spec, any_spec if layer == 0 else vm, any_spec, any_spec] + [any_spec] * 5
    aliases = {}
    if layer > 0:
        ins += list(prev)
        in_specs += [any_spec] * 2
        aliases = {9: 1, 10: 2}
    cache_t = jax.ShapeDtypeStruct(kc.shape, kc.dtype)
    return pl.pallas_call(
        functools.partial(attn_kernel, layer, n_steps, n_heads),
        out_shape=[jax.ShapeDtypeStruct((n_heads + 1, n_rows, head_dim), F32), cache_t, cache_t] + ([jax.ShapeDtypeStruct(u.shape, BF16)] if layer == 0 else []),
        in_specs=in_specs,
        out_specs=[vm, any_spec, any_spec] + ([vm] if layer == 0 else []),
        scratch_shapes=[
            pltpu.VMEM((d_model, q_cols), BF16), pltpu.VMEM((d_model, head_dim), BF16), pltpu.VMEM((d_model, head_dim), BF16),
            pltpu.VMEM((n_seq, n_slots, head_dim), BF16), pltpu.VMEM((n_seq, n_slots, head_dim), BF16),
            pltpu.VMEM((n_heads, n_rows, head_dim), F32), pltpu.VMEM((n_rows, head_dim), F32), pltpu.VMEM((n_rows, head_dim), F32),
            pltpu.SMEM(lengths.shape, jnp.int32), pltpu.VMEM(gain.shape, BF16), pltpu.VMEM(freq.shape, F32), pltpu.VMEM(u.shape if layer == 0 else (16, 128), BF16),
            pltpu.SemaphoreType.DMA((7,)), pltpu.SemaphoreType.DMA((2, n_seq // 2)), pltpu.SemaphoreType.DMA((2, n_seq // 2)),
        ],
        input_output_aliases=aliases,
        compiler_params=pltpu.CompilerParams(vmem_limit_bytes=ATTN_VMEM),
        name=f"attn{layer}",
    )(*ins)


def merge(a, b, n_heads):
    lane = lax.broadcasted_iota(jnp.int32, a(n_heads).shape, 1)
    st_a, st_b = a(n_heads), b(n_heads)
    m = jnp.maximum(st_a, st_b)
    fa, fb = jnp.exp(st_a - m), jnp.exp(st_b - m)
    fa = jnp.where(lane < 8, fa, 0.0)
    fb = jnp.where(lane < 8, fb, 0.0)
    l = st_a * pltpu.roll(fa, 8, 1) + st_b * pltpu.roll(fb, 8, 1)
    st = jnp.where(lane < 8, m, l)
    outs = [a(hd) * fa[:, hd:hd + 1] + b(hd) * fb[:, hd:hd + 1] for hd in range(n_heads)]
    return outs, st


def mix_kernel(layer, n_heads, part_ref, u_ref, gain_hbm, wo_hbm, wg_hbm, wu_hbm, wd_hbm, out_ref,
               wo_buf, wg_buf, wu_buf, wd_buf, core_in, fwd_out, fwd_in, y_out, y_in, u1_sc, h_out, h_in, hh, act,
               d_own, d_out, d_in, e_out, e_in, u_all, gain_ref, w_sem, send_sem, recv_sem):
    tp = lax.axis_index('tp')
    sp = lax.axis_index('sp')
    core = lax.rem(sp, 2)
    core_peer = {'sp': sp + 1 - 2 * core}
    far_peer = {'sp': lax.rem(sp + 2, 4)}
    tp_peer = {'tp': 1 - tp}
    n_blk, chunk, width = y_out.shape
    ff = wg_buf.shape[1]
    skip = 2 * ff - wg_hbm.shape[2]
    col0 = pl.multiple_of(core * (ff - skip), 128)

    w_copies = [
        pltpu.make_async_copy(wo_hbm.at[layer], wo_buf, w_sem.at[0]),
        pltpu.make_async_copy(wg_hbm.at[layer, :, pl.ds(col0, ff)], wg_buf, w_sem.at[1]),
        pltpu.make_async_copy(wu_hbm.at[layer, :, pl.ds(col0, ff)], wu_buf, w_sem.at[2]),
        pltpu.make_async_copy(wd_hbm.at[layer, pl.ds(col0, ff), :], wd_buf, w_sem.at[3]),
        pltpu.make_async_copy(gain_hbm, gain_ref, w_sem.at[4]),
    ]
    for cp in w_copies:
        cp.start()

    barrier = pltpu.get_barrier_semaphore()
    for peer in (core_peer, far_peer, tp_peer):
        pl.semaphore_signal(barrier, inc=1, device_id=peer, device_id_type=MESH)
    pl.semaphore_wait(barrier, 3)

    count = [0]

    def remote(src, dst, peer):
        k = count[0]
        count[0] += 1
        return pltpu.make_async_remote_copy(src_ref=src, dst_ref=dst, send_sem=send_sem.at[k], recv_sem=recv_sem.at[k], device_id=peer, device_id_type=MESH)

    def rows(idx):
        return pl.ds(pl.multiple_of(idx * chunk, chunk), chunk)

    far_chunk = lax.rem(sp + 2, 4)
    sib = sp + 1 - 2 * core
    sib_far = lax.rem(sib + 2, 4)

    c_far = remote(part_ref.at[:, rows(sib_far), :], core_in.at[0], core_peer)
    c_own = remote(part_ref.at[:, rows(sib), :], core_in.at[1], core_peer)
    c_far.start()
    c_own.start()
    fwd = remote(fwd_out, fwd_in, far_peer)
    c_far.wait_recv()
    outs, st = merge(lambda hd: part_ref[hd, rows(far_chunk), :], lambda hd: core_in[0, hd], n_heads)
    for hd in range(n_heads):
        fwd_out[hd] = outs[hd]
    fwd_out[n_heads] = st
    fwd.start()
    c_own.wait_recv()
    own, own_st = merge(lambda hd: part_ref[hd, rows(sp), :], lambda hd: core_in[1, hd], n_heads)
    for hd in range(n_heads):
        core_in[0, hd] = own[hd]
    core_in[0, n_heads] = own_st
    fwd.wait_recv()
    outs, st = merge(lambda hd: core_in[0, hd], lambda hd: fwd_in[hd], n_heads)
    attn_out = jnp.concatenate([(outs[hd] / st[:, 8 + hd:9 + hd]).astype(BF16) for hd in range(n_heads)], axis=1)

    y_copies = [remote(y_out.at[n], y_in.at[n], tp_peer) for n in range(n_blk)]
    w_copies[0].wait()
    w_copies[4].wait()
    for n in range(n_blk):
        y_out[n] = jnp.dot(attn_out, wo_buf[:, n * width:(n + 1) * width], preferred_element_type=F32)
        y_copies[n].start()
    for n in range(n_blk):
        y_copies[n].wait_recv()
        cols = slice(n * width, (n + 1) * width)
        u1_sc[:, cols] = (u_ref[rows(sp), cols].astype(F32) + (y_out[n] + y_in[n])).astype(BF16).astype(F32)
    h2 = rms_norm(u1_sc[...], gain_ref[layer:layer + 1, :].astype(F32))
    h_out[...] = h2.astype(F32)
    hh[0:chunk, :] = h2
    h_copy = remote(h_out, h_in, core_peer)
    h_copy.start()
    for cp in w_copies[1:4]:
        cp.wait()
    h_copy.wait_recv()
    hh[chunk:2 * chunk, :] = h_in[...].astype(BF16)

    blk = 256
    for n in range(ff // blk):
        cols = slice(n * blk, (n + 1) * blk)
        gate = jnp.dot(hh[...], wg_buf[:, cols], preferred_element_type=F32)
        up = jnp.dot(hh[...], wu_buf[:, cols], preferred_element_type=F32)
        val = gate / (1.0 + jnp.exp(-gate)) * up
        if n * blk < skip:
            lane = lax.broadcasted_iota(jnp.int32, val.shape, 1) + n * blk
            val = jnp.where(lane < skip * core, 0.0, val)
        act[:, cols] = val.astype(BF16)

    d_copies = [remote(d_out.at[n], d_in.at[n], core_peer) for n in range(n_blk)]
    e_copies = [remote(e_out.at[n], e_in.at[n], tp_peer) for n in range(n_blk)]
    a_core = [remote(u_all.at[n, rows(sp), :], u_all.at[n, rows(sp), :], core_peer) for n in range(n_blk)]
    a_far = [remote(u_all.at[n, rows(sp), :], u_all.at[n, rows(sp), :], far_peer) for n in range(n_blk)]
    a_fwd = [remote(u_all.at[n, rows(far_chunk), :], u_all.at[n, rows(far_chunk), :], core_peer) for n in range(n_blk)]
    for n in range(n_blk):
        down = jnp.dot(act[...], wd_buf[:, n * width:(n + 1) * width], preferred_element_type=F32)
        d_own[n] = down[:chunk]
        d_out[n] = down[chunk:]
        d_copies[n].start()
    for n in range(n_blk):
        d_copies[n].wait_recv()
        e_out[n] = d_own[n] + d_in[n]
        e_copies[n].start()
    for n in range(n_blk):
        e_copies[n].wait_recv()
        u_all[n, rows(sp), :] = (u1_sc[:, n * width:(n + 1) * width] + (e_out[n] + e_in[n])).astype(BF16).astype(F32)
        a_far[n].start()
        a_core[n].start()
    for n in range(n_blk):
        a_far[n].wait_recv()
        a_fwd[n].start()
    for n in range(n_blk):
        a_core[n].wait_recv()
        a_fwd[n].wait_recv()
        out_ref[:, n * width:(n + 1) * width] = u_all[n].astype(BF16)
    for cp in [c_far, c_own, fwd, h_copy] + y_copies + d_copies + e_copies + a_core + a_far + a_fwd:
        cp.wait_send()


def mix(layer, part, u, gain, w_out, w_gate, w_up, w_down):
    n_planes, n_rows, head_dim = part.shape
    n_heads = n_planes - 1
    d_model = u.shape[1]
    chunk = n_rows // 4
    n_tiles = w_gate.shape[2] // 128
    ff = ((n_tiles + 1) // 2) * 128
    n_blk = 6
    width = d_model // n_blk
    any_spec = pl.BlockSpec(memory_space=pltpu.HBM)
    vm = pl.BlockSpec(memory_space=pltpu.VMEM)
    blocks = pltpu.VMEM((n_blk, chunk, width), F32)
    planes = pltpu.VMEM((n_planes, chunk, head_dim), F32)
    n_copies = 4 + 6 * n_blk
    return pl.pallas_call(
        functools.partial(mix_kernel, layer, n_heads),
        out_shape=jax.ShapeDtypeStruct((n_rows, d_model), BF16),
        in_specs=[vm, vm] + [any_spec] * 5,
        out_specs=vm,
        scratch_shapes=[
            pltpu.VMEM((w_out.shape[1], d_model), BF16), pltpu.VMEM((d_model, ff), BF16), pltpu.VMEM((d_model, ff), BF16), pltpu.VMEM((ff, d_model), BF16),
            pltpu.VMEM((2, n_planes, chunk, head_dim), F32), planes, planes,
            blocks, blocks, pltpu.VMEM((chunk, d_model), F32), pltpu.VMEM((chunk, d_model), F32), pltpu.VMEM((chunk, d_model), F32),
            pltpu.VMEM((2 * chunk, d_model), BF16), pltpu.VMEM((2 * chunk, ff), BF16),
            blocks, blocks, blocks, blocks, blocks, pltpu.VMEM((n_blk, n_rows, width), F32),
            pltpu.VMEM(gain.shape, BF16), pltpu.SemaphoreType.DMA((5,)), pltpu.SemaphoreType.DMA((n_copies,)), pltpu.SemaphoreType.DMA((n_copies,)),
        ],
        compiler_params=pltpu.CompilerParams(collective_id=layer, has_side_effects=True, vmem_limit_bytes=MIX_VMEM),
        name=f"mix{layer}",
    )(part, u, gain, w_out, w_gate, w_up, w_down)


def in_hbm(x):
    return pltpu.with_memory_space_constraint(x, pltpu.HBM)


def solution(mesh):
    def local_fn(tok_emb, lengths, key_cache, val_cache, gain_attn, gain_mlp, w_query, w_key, w_value, w_out, w_gate, w_up, w_down):
        n_steps, n_batch, d_model = tok_emb.shape
        n_layers, _, loc_len, kv_loc, head_dim = key_cache.shape
        n_rows = n_steps * n_batch
        kc = key_cache.reshape(n_layers, n_batch, loc_len, head_dim)
        vc = val_cache.reshape(n_layers, n_batch, loc_len, head_dim)
        half = np.arange(head_dim // 2, dtype=np.float32) * np.float32(2.0) / np.float32(head_dim)
        freq = np.float32(1.0) / np.power(np.float32(ROPE_BASE), half)
        freq = jnp.asarray(np.concatenate([freq, freq])[None], F32)
        u = tok_emb.reshape(n_rows, d_model)
        u, lengths, freq, gain_attn, gain_mlp, kc, vc = map(in_hbm, (u, lengths, freq, gain_attn, gain_mlp, kc, vc))
        w_query, w_key, w_value, w_out, w_gate, w_up, w_down = map(in_hbm, (w_query, w_key, w_value, w_out, w_gate, w_up, w_down))
        prev = None
        for layer in range(n_layers):
            res = attention(layer, n_steps, lengths, u, gain_attn, freq, w_query, w_key, w_value, kc, vc, prev)
            part, prev = res[0], res[1:3]
            if layer == 0:
                u = res[3]
            u = mix(layer, part, u, gain_mlp, w_out, w_gate, w_up, w_down)
        hidden = u.reshape(n_batch, n_steps, d_model).transpose(1, 0, 2)
        return hidden, prev[0].reshape(key_cache.shape), prev[1].reshape(val_cache.shape)

    cache_spec = P(None, 'dp', 'sp', 'tp', None)
    col_spec = P(None, None, 'tp')
    row_spec = P(None, 'tp', None)
    emb_spec = P(None, 'dp', None)
    return jax.shard_map(local_fn, mesh=mesh, in_specs=(emb_spec, P('dp'), cache_spec, cache_spec, P(), P(), col_spec, col_spec, col_spec, row_spec, col_spec, col_spec, row_spec), out_specs=(emb_spec, cache_spec, cache_spec), check_vma=False)
```

```python
import functools
import jax
import jax.numpy as jnp
import numpy as np
from jax import lax
from jax.experimental import pallas as pl
from jax.experimental.pallas import tpu as pltpu
from jax.sharding import PartitionSpec as P

EPS = 1e-5
ROPE_BASE = 500000.0
F32 = jnp.float32
BF16 = jnp.bfloat16
MESH = pl.DeviceIdType.MESH


def rms_norm(x_float, gain_row):
    inv_rms = lax.rsqrt(jnp.mean(x_float * x_float, axis=-1, keepdims=True) + EPS)
    return (x_float * inv_rms * gain_row).astype(BF16)


def attn_kernel(layer, n_steps, n_heads, names, *refs):
    r = dict(zip(names, refs))
    len_ref, gain_ref, freq_ref, q_sc, kn_sc, vn_sc, o_ref = (r[k] for k in ('len', 'gain', 'freq', 'q_sc', 'kn_sc', 'vn_sc', 'part'))
    kbuf, vbuf, wq_buf, wk_buf, wv_buf, w_sem, in_sem, out_sem = (r[k] for k in ('kbuf', 'vbuf', 'wq_buf', 'wk_buf', 'wv_buf', 'w_sem', 'in_sem', 'out_sem'))
    ko_hbm, vo_hbm = r['ko'], r['vo']
    u_in = r['u_in']
    sp = lax.axis_index('sp')
    n_rows = u_in.shape[0]
    n_slots, head_dim = kbuf.shape[1], kbuf.shape[2]
    n_seq = kbuf.shape[0]
    n_pairs = n_seq // 2
    pair_rows = 2 * n_steps
    first_layer = layer == 0

    copies = [(r['len_in'], len_ref), (r['gain_in'], gain_ref)]
    if first_layer:
        copies += [(r['freq_in'], freq_ref), (u_in, r['u_buf']), (r['wq_in'].at[layer], wq_buf), (r['wk_in'].at[layer], wk_buf), (r['wv_in'].at[layer], wv_buf)]
    copies = [pltpu.make_async_copy(src, dst, w_sem.at[i]) for i, (src, dst) in enumerate(copies)]
    smalls, w_copies = copies[:4], copies[4:]
    for cp in copies:
        cp.start()

    def in_copies(i):
        sl = pl.ds(2 * i, 2)
        return (pltpu.make_async_copy(r['kc'].at[layer, sl], kbuf.at[sl], in_sem.at[0, i]),
                pltpu.make_async_copy(r['vc'].at[layer, sl], vbuf.at[sl], in_sem.at[1, i]))

    def out_copies(i):
        sl = pl.ds(2 * i, 2)
        return (pltpu.make_async_copy(kbuf.at[sl], ko_hbm.at[layer, sl], out_sem.at[0]),
                pltpu.make_async_copy(vbuf.at[sl], vo_hbm.at[layer, sl], out_sem.at[1]))

    if first_layer:
        @pl.loop(0, n_pairs)
        def _(i):
            for cp in in_copies(i):
                cp.start()

    for cp in smalls:
        cp.wait()
    if first_layer:
        row = lax.broadcasted_iota(jnp.int32, (n_rows, n_rows), 0)
        col = lax.broadcasted_iota(jnp.int32, (n_rows, n_rows), 1)
        perm = jnp.where(col == (row % n_steps) * n_seq + row // n_steps, 1.0, 0.0).astype(BF16)
        u = jnp.dot(perm, r['u_buf'][...], preferred_element_type=F32)
        r['u_perm'][...] = u.astype(BF16)
    else:
        u = u_in[...].astype(F32)
    h = rms_norm(u, gain_ref[layer:layer + 1, :].astype(F32))
    cos_ref, sin_ref = r['cos'], r['sin']
    if first_layer:
        sub8 = lax.broadcasted_iota(jnp.int32, (pair_rows, head_dim), 0)
        pos = jnp.concatenate([jnp.where(sub8 < n_steps, len_ref[2 * i], len_ref[2 * i + 1]) + sub8 % n_steps for i in range(n_pairs)], axis=0)
        angles = pos.astype(F32) * freq_ref[...]
        lane = lax.broadcasted_iota(jnp.int32, angles.shape, 1)
        cos_ref[...] = jnp.cos(angles)
        sin_t = jnp.sin(angles)
        sin_ref[...] = jnp.where(lane < head_dim // 2, -sin_t, sin_t)
    cos_t = cos_ref[...]
    sin_t = sin_ref[...]

    def rope(x):
        return (x * cos_t + pltpu.roll(x, head_dim // 2, 1) * sin_t).astype(BF16).astype(F32)

    for cp in w_copies:
        cp.wait()
    q_all = jnp.dot(h, wq_buf[...], preferred_element_type=F32)
    for hd in range(n_heads):
        q_sc[hd] = rope(q_all[:, hd * head_dim:(hd + 1) * head_dim])
    kn_sc[...] = rope(jnp.dot(h, wk_buf[...], preferred_element_type=F32))
    vn_sc[...] = jnp.dot(h, wv_buf[...], preferred_element_type=F32).astype(BF16).astype(F32)

    m_rows = n_heads * pair_rows
    scale = head_dim ** -0.5

    def pair_body(i):
        if first_layer:
            for cp in in_copies(i):
                cp.wait()
        sub = lax.broadcasted_iota(jnp.int32, (m_rows, 1), 0) % pair_rows
        first = sub < n_steps
        q48 = jnp.concatenate([q_sc[hd, pl.ds(pair_rows * i, pair_rows), :] for hd in range(n_heads)], axis=0).astype(BF16)
        scs = []
        for e in range(2):
            b = 2 * i + e
            step = (len_ref[b] + (4 - sp)) & 3
            step = (4 - step) & 3
            slot = (len_ref[b] + step) // 4
            row = n_steps * b + step
            base = pl.multiple_of((slot // 16) * 16, 16)
            hit = lax.broadcasted_iota(jnp.int32, (16, head_dim), 0) == slot - base
            for buf, new in ((kbuf, kn_sc), (vbuf, vn_sc)):
                tile = buf[b, pl.ds(base, 16), :].astype(F32)
                new_row = new[pl.ds(row, 1), :]
                buf[b, pl.ds(base, 16), :] = jnp.where(hit, jnp.broadcast_to(new_row, (16, head_dim)), tile).astype(BF16)
            scs.append(lax.dot_general(q48, kbuf[b], (((1,), (1,)), ((), ())), preferred_element_type=F32))
        lim = (jnp.where(first, len_ref[2 * i] + sub, len_ref[2 * i + 1] + sub - n_steps) - sp) // 4
        s = jnp.where(jnp.broadcast_to(first, scs[0].shape), scs[0], scs[1]) * scale
        slot_id = lax.broadcasted_iota(jnp.int32, s.shape, 1)
        s = jnp.where(slot_id <= lim, s, -1e30)
        m = jnp.max(s, axis=-1, keepdims=True)
        p = jnp.exp(s - m)
        l = jnp.sum(p, axis=-1, keepdims=True)
        pb = p.astype(BF16)
        o0 = jnp.dot(pb, vbuf[2 * i], preferred_element_type=F32)
        o1 = jnp.dot(pb, vbuf[2 * i + 1], preferred_element_type=F32)
        o = jnp.where(jnp.broadcast_to(first, o0.shape), o0, o1)
        lane = lax.broadcasted_iota(jnp.int32, (pair_rows, head_dim), 1)
        st = jnp.zeros((pair_rows, head_dim), F32)
        for hd in range(n_heads):
            rs = slice(hd * pair_rows, (hd + 1) * pair_rows)
            o_ref[hd, pl.ds(pair_rows * i, pair_rows), :] = o[rs]
            st = jnp.where(lane == hd, m[rs], jnp.where(lane == hd + 8, l[rs], st))
        o_ref[n_heads, pl.ds(pair_rows * i, pair_rows), :] = st
        for cp in out_copies(i):
            cp.start()

    @pl.loop(0, n_pairs // 2)
    def _(i):
        pair_body(2 * i)
        pair_body(2 * i + 1)

    @pl.loop(0, n_pairs)
    def _(i):
        for cp in out_copies(i):
            cp.wait()


def attention(layer, n_steps, n_heads, lengths, u, gain, ins):
    n_rows, d_model = u.shape
    head_dim = 128
    hbm = pl.BlockSpec(memory_space=pltpu.HBM)
    vm = pl.BlockSpec(memory_space=pltpu.VMEM)
    first_layer = layer == 0
    n_seq = n_rows // n_steps
    tile = jax.ShapeDtypeStruct((n_rows, head_dim), F32)
    part = jax.ShapeDtypeStruct((n_heads + 1, n_rows, head_dim), F32)
    scratch = {'len': pltpu.SMEM(lengths.shape, jnp.int32), 'gain': pltpu.VMEM(gain.shape, BF16), 'q_sc': pltpu.VMEM((n_heads, n_rows, head_dim), F32),
               'kn_sc': pltpu.VMEM((n_rows, head_dim), F32), 'vn_sc': pltpu.VMEM((n_rows, head_dim), F32), 'w_sem': pltpu.SemaphoreType.DMA((7,)), 'out_sem': pltpu.SemaphoreType.DMA((2,))}
    if first_layer:
        freq, w_query, w_key, w_value, kc, vc = ins
        cache_t = jax.ShapeDtypeStruct(kc.shape, kc.dtype)
        args = {'len_in': lengths, 'u_in': u, 'gain_in': gain, 'freq_in': freq, 'wq_in': w_query, 'wk_in': w_key, 'wv_in': w_value, 'kc': kc, 'vc': vc}
        specs = {k: hbm for k in args}
        outs = {'part': (part, vm), 'ko': (cache_t, hbm), 'vo': (cache_t, hbm), 'u_perm': (jax.ShapeDtypeStruct(u.shape, BF16), vm), 'cos': (tile, vm), 'sin': (tile, vm)}
        scratch.update({'freq': pltpu.VMEM(freq.shape, F32), 'u_buf': pltpu.VMEM(u.shape, BF16), 'kbuf': pltpu.VMEM(kc.shape[1:], BF16), 'vbuf': pltpu.VMEM(kc.shape[1:], BF16),
                        'wq_buf': pltpu.VMEM(w_query.shape[1:], BF16), 'wk_buf': pltpu.VMEM(w_key.shape[1:], BF16), 'wv_buf': pltpu.VMEM(w_value.shape[1:], BF16),
                        'in_sem': pltpu.SemaphoreType.DMA((2, n_seq // 2))})
        aliases = {}
    else:
        cos_t, sin_t, ko, vo, k_loc, v_loc, wq, wk, wv = ins
        cache_t = jax.ShapeDtypeStruct(ko.shape, ko.dtype)
        loc_t = pltpu.VMEM(k_loc.shape, BF16)
        k_loc, v_loc, wq, wk, wv = map(in_vmem, (k_loc, v_loc, wq, wk, wv))
        args = {'len_in': lengths, 'u_in': u, 'gain_in': gain, 'cos': cos_t, 'sin': sin_t, 'wq_buf': wq, 'wk_buf': wk, 'wv_buf': wv, 'ko_in': ko, 'vo_in': vo, 'k_loc': k_loc, 'v_loc': v_loc}
        specs = {k: hbm if k in ('len_in', 'gain_in', 'ko_in', 'vo_in') else vm for k in args}
        outs = {'part': (part, vm), 'ko': (cache_t, hbm), 'vo': (cache_t, hbm), 'kbuf': (loc_t, vm), 'vbuf': (loc_t, vm)}
        scratch.update({'freq': pltpu.SMEM((1,), jnp.int32), 'in_sem': pltpu.SemaphoreType.DMA((1,))})
        order = list(args)
        aliases = {order.index('ko_in'): 1, order.index('vo_in'): 2, order.index('k_loc'): 3, order.index('v_loc'): 4}
    names = list(args) + list(outs) + list(scratch)
    res = pl.pallas_call(
        functools.partial(attn_kernel, layer, n_steps, n_heads, names),
        out_shape=[o[0] for o in outs.values()],
        in_specs=list(specs.values()),
        out_specs=[o[1] for o in outs.values()],
        scratch_shapes=list(scratch.values()),
        input_output_aliases=aliases,
        compiler_params=pltpu.CompilerParams(vmem_limit_bytes=(32 if first_layer else 8) * 1024 * 1024),
        name=f"attn{layer}",
    )(*args.values())
    return dict(zip(outs, res))


def merge(a, b, n_heads):
    lane = lax.broadcasted_iota(jnp.int32, a(n_heads).shape, 1)
    st_a, st_b = a(n_heads), b(n_heads)
    m = jnp.maximum(st_a, st_b)
    fa, fb = jnp.exp(st_a - m), jnp.exp(st_b - m)
    fa = jnp.where(lane < 8, fa, 0.0)
    fb = jnp.where(lane < 8, fb, 0.0)
    l = st_a * pltpu.roll(fa, 8, 1) + st_b * pltpu.roll(fb, 8, 1)
    st = jnp.where(lane < 8, m, l)
    outs = [a(hd) * fa[:, hd:hd + 1] + b(hd) * fb[:, hd:hd + 1] for hd in range(n_heads)]
    return outs, st


def mix_kernel(layer, n_heads, n_next, part_ref, u_ref, gain_hbm, wo_hbm, wg_hbm, wu_hbm, wd_hbm, *rest):
    next_src, out_ref, next_dst, rest = rest[:n_next], rest[n_next], rest[n_next + 1:2 * n_next + 1], rest[2 * n_next + 1:]
    mix_body(layer, n_heads, part_ref, u_ref, gain_hbm, wo_hbm, wg_hbm, wu_hbm, wd_hbm, next_src, next_dst, out_ref, *rest)


def mix_body(layer, n_heads, part_ref, u_ref, gain_hbm, wo_hbm, wg_hbm, wu_hbm, wd_hbm, next_src, next_dst, out_ref,
               wo_buf, wg_buf, wu_buf, wd_buf, core_in, fwd_out, fwd_in, y_out, y_in, u1_sc, h_out, h_in, hh, act,
               d_own, d_out, d_in, e_out, e_in, u_all, gain_ref, w_sem, send_sem, recv_sem):
    tp = lax.axis_index('tp')
    sp = lax.axis_index('sp')
    core = lax.rem(sp, 2)
    core_peer = {'sp': sp + 1 - 2 * core}
    far_peer = {'sp': lax.rem(sp + 2, 4)}
    tp_peer = {'tp': 1 - tp}
    n_blk, chunk, width = y_out.shape
    ff = wg_buf.shape[1]
    skip = 2 * ff - wg_hbm.shape[2]
    col0 = pl.multiple_of(core * (ff - skip), 128)

    w_copies = [
        pltpu.make_async_copy(wo_hbm.at[layer], wo_buf, w_sem.at[0]),
        pltpu.make_async_copy(wg_hbm.at[layer, :, pl.ds(col0, ff)], wg_buf, w_sem.at[1]),
        pltpu.make_async_copy(wu_hbm.at[layer, :, pl.ds(col0, ff)], wu_buf, w_sem.at[2]),
        pltpu.make_async_copy(wd_hbm.at[layer, pl.ds(col0, ff), :], wd_buf, w_sem.at[3]),
        pltpu.make_async_copy(gain_hbm, gain_ref, w_sem.at[4]),
    ]
    pre_copies = [pltpu.make_async_copy(src.at[layer + 1], dst, w_sem.at[5 + i]) for i, (src, dst) in enumerate(zip(next_src, next_dst))]
    for cp in w_copies + pre_copies:
        cp.start()

    barrier = pltpu.get_barrier_semaphore()
    for peer in (core_peer, far_peer, tp_peer):
        pl.semaphore_signal(barrier, inc=1, device_id=peer, device_id_type=MESH)
    pl.semaphore_wait(barrier, 3)

    count = [0]

    def remote(src, dst, peer):
        k = count[0]
        count[0] += 1
        return pltpu.make_async_remote_copy(src_ref=src, dst_ref=dst, send_sem=send_sem.at[k], recv_sem=recv_sem.at[k], device_id=peer, device_id_type=MESH)

    def rows(idx):
        return pl.ds(pl.multiple_of(idx * chunk, chunk), chunk)

    far_chunk = lax.rem(sp + 2, 4)
    sib = sp + 1 - 2 * core
    sib_far = lax.rem(sib + 2, 4)

    c_far = remote(part_ref.at[:, rows(sib_far), :], core_in.at[0], core_peer)
    c_own = remote(part_ref.at[:, rows(sib), :], core_in.at[1], core_peer)
    c_far.start()
    c_own.start()
    fwd = remote(fwd_out, fwd_in, far_peer)
    c_far.wait_recv()
    outs, st = merge(lambda hd: part_ref[hd, rows(far_chunk), :], lambda hd: core_in[0, hd], n_heads)
    for hd in range(n_heads):
        fwd_out[hd] = outs[hd]
    fwd_out[n_heads] = st
    fwd.start()
    c_own.wait_recv()
    own, own_st = merge(lambda hd: part_ref[hd, rows(sp), :], lambda hd: core_in[1, hd], n_heads)
    for hd in range(n_heads):
        core_in[0, hd] = own[hd]
    core_in[0, n_heads] = own_st
    fwd.wait_recv()
    outs, st = merge(lambda hd: core_in[0, hd], lambda hd: fwd_in[hd], n_heads)
    attn_out = jnp.concatenate([(outs[hd] / st[:, 8 + hd:9 + hd]).astype(BF16) for hd in range(n_heads)], axis=1)

    y_copies = [remote(y_out.at[n], y_in.at[n], tp_peer) for n in range(n_blk)]
    w_copies[0].wait()
    w_copies[4].wait()
    for n in range(n_blk):
        y_out[n] = jnp.dot(attn_out, wo_buf[:, n * width:(n + 1) * width], preferred_element_type=F32)
        y_copies[n].start()
    for n in range(n_blk):
        y_copies[n].wait_recv()
        cols = slice(n * width, (n + 1) * width)
        u1_sc[:, cols] = (u_ref[rows(sp), cols].astype(F32) + (y_out[n] + y_in[n])).astype(BF16).astype(F32)
    h2 = rms_norm(u1_sc[...], gain_ref[layer:layer + 1, :].astype(F32))
    h_out[...] = h2.astype(F32)
    hh[0:chunk, :] = h2
    h_copy = remote(h_out, h_in, core_peer)
    h_copy.start()
    for cp in w_copies[1:4]:
        cp.wait()
    h_copy.wait_recv()
    hh[chunk:2 * chunk, :] = h_in[...].astype(BF16)

    blk = 256
    for n in range(ff // blk):
        cols = slice(n * blk, (n + 1) * blk)
        gate = jnp.dot(hh[...], wg_buf[:, cols], preferred_element_type=F32)
        up = jnp.dot(hh[...], wu_buf[:, cols], preferred_element_type=F32)
        val = gate / (1.0 + jnp.exp(-gate)) * up
        if n * blk < skip:
            lane = lax.broadcasted_iota(jnp.int32, val.shape, 1) + n * blk
            val = jnp.where(lane < skip * core, 0.0, val)
        act[:, cols] = val.astype(BF16)

    d_copies = [remote(d_out.at[n], d_in.at[n], core_peer) for n in range(n_blk)]
    e_copies = [remote(e_out.at[n], e_in.at[n], tp_peer) for n in range(n_blk)]
    a_core = [remote(u_all.at[n, rows(sp), :], u_all.at[n, rows(sp), :], core_peer) for n in range(n_blk)]
    a_far = [remote(u_all.at[n, rows(sp), :], u_all.at[n, rows(sp), :], far_peer) for n in range(n_blk)]
    a_fwd = [remote(u_all.at[n, rows(far_chunk), :], u_all.at[n, rows(far_chunk), :], core_peer) for n in range(n_blk)]
    for n in range(n_blk):
        down = jnp.dot(act[...], wd_buf[:, n * width:(n + 1) * width], preferred_element_type=F32)
        d_own[n] = down[:chunk]
        d_out[n] = down[chunk:]
        d_copies[n].start()
    for n in range(n_blk):
        d_copies[n].wait_recv()
        e_out[n] = d_own[n] + d_in[n]
        e_copies[n].start()
    for n in range(n_blk):
        e_copies[n].wait_recv()
        u_all[n, rows(sp), :] = (u1_sc[:, n * width:(n + 1) * width] + (e_out[n] + e_in[n])).astype(BF16).astype(F32)
        a_far[n].start()
        a_core[n].start()
    for n in range(n_blk):
        a_far[n].wait_recv()
        a_fwd[n].start()
    for n in range(n_blk):
        a_core[n].wait_recv()
        a_fwd[n].wait_recv()
        out_ref[:, n * width:(n + 1) * width] = u_all[n].astype(BF16)
    for cp in pre_copies:
        cp.wait()
    for cp in [c_far, c_own, fwd, h_copy] + y_copies + d_copies + e_copies + a_core + a_far + a_fwd:
        cp.wait_send()


def mix(layer, part, u, gain, w_out, w_gate, w_up, w_down, nxt):
    n_planes, n_rows, head_dim = part.shape
    n_heads = n_planes - 1
    d_model = u.shape[1]
    chunk = n_rows // 4
    n_tiles = w_gate.shape[2] // 128
    ff = ((n_tiles + 1) // 2) * 128
    n_blk = 3
    width = d_model // n_blk
    hbm = pl.BlockSpec(memory_space=pltpu.HBM)
    vm = pl.BlockSpec(memory_space=pltpu.VMEM)
    blocks = pltpu.VMEM((n_blk, chunk, width), F32)
    planes = pltpu.VMEM((n_planes, chunk, head_dim), F32)
    n_copies = 4 + 6 * n_blk
    return pl.pallas_call(
        functools.partial(mix_kernel, layer, n_heads, len(nxt)),
        out_shape=[jax.ShapeDtypeStruct((n_rows, d_model), BF16)] + [pltpu.VMEM(w.shape[1:], w.dtype) for w in nxt],
        in_specs=[vm, vm] + [hbm] * (5 + len(nxt)),
        out_specs=[vm] * (1 + len(nxt)),
        scratch_shapes=[
            pltpu.VMEM((w_out.shape[1], d_model), BF16), pltpu.VMEM((d_model, ff), BF16), pltpu.VMEM((d_model, ff), BF16), pltpu.VMEM((ff, d_model), BF16),
            pltpu.VMEM((2, n_planes, chunk, head_dim), F32), planes, planes,
            blocks, blocks, pltpu.VMEM((chunk, d_model), F32), pltpu.VMEM((chunk, d_model), F32), pltpu.VMEM((chunk, d_model), F32),
            pltpu.VMEM((2 * chunk, d_model), BF16), pltpu.VMEM((2 * chunk, ff), BF16),
            blocks, blocks, blocks, blocks, blocks, pltpu.VMEM((n_blk, n_rows, width), F32),
            pltpu.VMEM(gain.shape, BF16), pltpu.SemaphoreType.DMA((5 + len(nxt),)), pltpu.SemaphoreType.DMA((n_copies,)), pltpu.SemaphoreType.DMA((n_copies,)),
        ],
        compiler_params=pltpu.CompilerParams(collective_id=layer, has_side_effects=True, vmem_limit_bytes=32 * 1024 * 1024),
        name=f"mix{layer}",
    )(part, u, gain, w_out, w_gate, w_up, w_down, *nxt)


def in_hbm(x):
    return pltpu.with_memory_space_constraint(x, pltpu.HBM)


def in_vmem(x):
    return pltpu.with_memory_space_constraint(x, pltpu.VMEM)


def solution(mesh):
    def local_fn(tok_emb, lengths, key_cache, val_cache, gain_attn, gain_mlp, w_query, w_key, w_value, w_out, w_gate, w_up, w_down):
        n_steps, n_batch, d_model = tok_emb.shape
        n_layers, _, loc_len, kv_loc, head_dim = key_cache.shape
        n_rows = n_steps * n_batch
        kc = key_cache.reshape(n_layers, n_batch, loc_len, head_dim)
        vc = val_cache.reshape(n_layers, n_batch, loc_len, head_dim)
        half = np.arange(head_dim // 2, dtype=np.float32) * np.float32(2.0) / np.float32(head_dim)
        freq = np.float32(1.0) / np.power(np.float32(ROPE_BASE), half)
        freq = jnp.asarray(np.concatenate([freq, freq])[None], F32)
        u = tok_emb.reshape(n_rows, d_model)
        u, lengths, freq, gain_attn, gain_mlp, kc, vc = map(in_hbm, (u, lengths, freq, gain_attn, gain_mlp, kc, vc))
        w_query, w_key, w_value, w_out, w_gate, w_up, w_down = map(in_hbm, (w_query, w_key, w_value, w_out, w_gate, w_up, w_down))
        n_heads = w_query.shape[2] // head_dim
        nxt = [kc, vc, w_query, w_key, w_value]
        res = attention(0, n_steps, n_heads, lengths, u, gain_attn, (freq, w_query, w_key, w_value, kc, vc))
        u, *loc = mix(0, res['part'], res['u_perm'], gain_mlp, w_out, w_gate, w_up, w_down, nxt)
        res = attention(1, n_steps, n_heads, lengths, u, gain_attn, (res['cos'], res['sin'], res['ko'], res['vo'], *loc))
        u, = mix(1, res['part'], u, gain_mlp, w_out, w_gate, w_up, w_down, [])
        prev = (res['ko'], res['vo'])
        hidden = u.reshape(n_batch, n_steps, d_model).transpose(1, 0, 2)
        return hidden, prev[0].reshape(key_cache.shape), prev[1].reshape(val_cache.shape)

    cache_spec = P(None, 'dp', 'sp', 'tp', None)
    col_spec = P(None, None, 'tp')
    row_spec = P(None, 'tp', None)
    emb_spec = P(None, 'dp', None)
    return jax.shard_map(local_fn, mesh=mesh, in_specs=(emb_spec, P('dp'), cache_spec, cache_spec, P(), P(), col_spec, col_spec, col_spec, row_spec, col_spec, col_spec, row_spec), out_specs=(emb_spec, cache_spec, cache_spec), check_vma=False)
```
